128 devices in a mesh: seq: 32 (over z, y, core), chan: 4 (over x).
Axes of the slice: x: 4, y: 4, z: 4, core: 2. Of those that a mesh axis runs over, the one named last changes fastest.
Arguments:
- features: bfloat16 [393216, 1024], P('seq', 'chan'), may hold values from -6 to 6
- gate_input: bfloat16 [393216, 1024], P('seq', 'chan'), may hold values from -6 to 6
- input_map: bfloat16 [393216, 128], P('seq', 'chan'), may hold values from -6 to 6
- output_map: bfloat16 [393216, 128], P('seq', 'chan'), may hold values from -6 to 6
- step_raw: float32 [393216, 16], P('seq', 'chan'), may hold values from -4 to 4
- step_bias: float32 [16], P('chan')
- decay_log: float32 [16], P('chan')
- skip_gain: float32 [16], P('chan'), may hold values from 0.5 to 1.5
- norm_gain: float32 [1024], P('chan'), may hold values from 0.1 to 1.9
- tissue: int32 [768, 2], P('seq'), may hold values from 0 to 512, as said below
Outputs:
- mixed: bfloat16 [393216, 1024], P('seq', 'chan')
The draws below stay inside these ranges and needn't reach their ends.
Inputs may be any that keep to these rules, and one draw needn't show every extreme that they name: tissue[r, 0] <= tissue[r, 1]; a row with equal values holds no tissue.
All inputs are finite; a program needn't handle non-finite values.
Results may differ from the reference program's by a relative error of at most 0.0039.
Values may be sent and summed in bfloat16 or wider, within the bound.
A program may use at most 192 MiB of HBM per device.

```python
import jax
import jax.numpy as jnp
from jax import lax

D = 1024
HEAD = 64
STATE = 128
ROW = 512
HEADS = 16
TOKENS = 393216


def head_kinds(key):
    share = 0.5
    return jax.random.uniform(jax.random.fold_in(key, 11), (HEADS,), jnp.float32) < share


def draw_step_bias(key, part):
    slow = head_kinds(key)
    spread = jax.random.uniform(jax.random.fold_in(key, 21), (HEADS,), jnp.float32)
    return jnp.where(slow, -9.5 + 1.3 * spread, -4.2 + 1.4 * spread).astype(jnp.float32)


def draw_decay_log(key, part):
    slow = head_kinds(key)
    spread = jax.random.uniform(jax.random.fold_in(key, 31), (HEADS,), jnp.float32)
    fast_log = -0.7 + 1.4 * spread
    slow_log = jnp.log((0.5 + spread) / (TOKENS * 0.0001))
    return jnp.where(slow, slow_log, fast_log).astype(jnp.float32)


def draw_tissue(key, part):
    row_count = TOKENS // ROW
    first = jax.random.randint(jax.random.fold_in(key, 41), (row_count,), 0, ROW // 2 + 1)
    last = jax.random.randint(jax.random.fold_in(key, 42), (row_count,), ROW // 2, ROW + 1)
    empty = jax.random.randint(jax.random.fold_in(key, 43), (row_count,), 0, 4) == 0
    last = jnp.where(empty, first, last)
    return jnp.stack([first, last], axis=1).astype(jnp.int32)


def shard_levels(key, dims, cuts, smallest, largest):
    def one(axis_at, shards_of):
        draws = jax.random.uniform(jax.random.fold_in(jax.random.fold_in(key, 6), axis_at), (shards_of,), jnp.float32, smallest / len(cuts), largest / len(cuts))
        return jnp.repeat(jnp.exp(draws), dims[axis_at] // shards_of).reshape((-1,) + (1,) * (len(dims) - axis_at - 1))

    gain = one(*cuts[0])
    for cut in cuts[1:]:
        gain = gain * one(*cut)
    return gain


def scatter_about(rng, extent, scale, most, cuts=(), kind=jnp.bfloat16):
    values = scale * jax.random.normal(rng, extent, jnp.float32)
    if cuts:
        values = values * shard_levels(rng, extent, cuts, -0.22, 0.18)
    return jnp.clip(values, -most, most).astype(kind)


def setup_inputs(seed: int = 0) -> dict:
    splits = jax.random.split(jax.random.key(seed), 11)
    return {
        "features": scatter_about(splits[0], (TOKENS, D), 1.0, 6.0, ((0, 32), (1, 4))),
        "gate_input": scatter_about(splits[1], (TOKENS, D), 1.0, 6.0, ((0, 32), (1, 4))),
        "input_map": scatter_about(splits[2], (TOKENS, STATE), 1.0, 6.0, ((0, 32), (1, 4))),
        "output_map": scatter_about(splits[3], (TOKENS, STATE), 1.0, 6.0, ((0, 32), (1, 4))),
        "step_raw": scatter_about(splits[4], (TOKENS, HEADS), 0.7, 4.0, ((0, 32), (1, 4)), jnp.float32),
        "step_bias": draw_step_bias(jax.random.fold_in(splits[10], 71), 0),
        "decay_log": draw_decay_log(jax.random.fold_in(splits[10], 71), 0),
        "skip_gain": jnp.clip(0.5 + 1.0 * jax.random.uniform(splits[7], (HEADS,), jnp.float32) ** shard_levels(splits[7], (HEADS,), ((0, 4),), -0.2, 0.2), 0.5, 1.5),
        "norm_gain": jnp.clip(1.0 + 0.18 * jax.random.normal(splits[8], (D,), jnp.float32), 0.1, 1.9),
        "tissue": draw_tissue(jax.random.fold_in(splits[10], 71), 0),
    }


EPS = 1e-05

def row_block(state_in, items):
    x_row, gate_row, b_row, c_row, log_row, step_row = items
    running = jnp.cumsum(log_row, axis=0)
    length = log_row.shape[0]
    order = jnp.arange(length, dtype=jnp.int32)
    causal = (order[:, None] >= order[None, :])[None]
    scores = jnp.dot(c_row, b_row.T, preferred_element_type=jnp.float32)
    per_head = running.T
    gap_log = per_head[:, :, None] - per_head[:, None, :]
    damping = jnp.where(causal, jnp.exp(jnp.where(causal, gap_log, 0.0)), 0.0)
    weights = (scores[None] * damping * step_row.T[:, None, :]).astype(jnp.bfloat16)
    x_wide = x_row.astype(jnp.float32)
    inner = jnp.einsum('hts,shp->thp', weights.astype(jnp.float32), x_wide, precision=lax.Precision.HIGHEST)
    carried = jnp.exp(running)[:, :, None] * jnp.einsum('tn,hnp->thp', c_row.astype(jnp.float32), state_in, precision=lax.Precision.HIGHEST)
    row_total = running[-1]
    scaled = jnp.exp(row_total[None, :] - running) * step_row
    b_scaled = (scaled.T[:, :, None] * b_row.astype(jnp.float32)[None]).astype(jnp.bfloat16)
    state_out = jnp.exp(row_total)[:, None, None] * state_in + jnp.einsum('hsn,shp->hnp', b_scaled.astype(jnp.float32), x_wide, precision=lax.Precision.HIGHEST)
    return (state_out, (inner + carried, gate_row))

def reference(features, gate_input, input_map, output_map, step_raw, step_bias, decay_log, skip_gain, norm_gain, tissue):
    row_count = TOKENS // ROW
    position = jnp.arange(ROW, dtype=jnp.int32)
    inside = ((position[None, :] >= tissue[:, 0:1]) & (position[None, :] < tissue[:, 1:2])).astype(jnp.float32)
    step_size = jax.nn.softplus(step_raw.reshape(row_count, ROW, HEADS) + step_bias) * inside[:, :, None]
    log_decay = -jnp.exp(decay_log) * step_size
    x_rows = features.reshape(row_count, ROW, HEADS, HEAD)
    gate_rows = gate_input.reshape(row_count, ROW, D)
    b_rows = input_map.reshape(row_count, ROW, STATE)
    c_rows = output_map.reshape(row_count, ROW, STATE)
    start = jnp.zeros((HEADS, STATE, HEAD), jnp.float32)

    def one_row(state_in, items):
        state_out, (scan_row, gate_row) = row_block(state_in, items)
        y_row = scan_row + skip_gain[:, None] * items[0].astype(jnp.float32)
        gated = y_row.reshape(ROW, D) * jax.nn.silu(gate_row.astype(jnp.float32))
        mean_square = lax.optimization_barrier(jnp.mean(gated * gated, axis=-1, keepdims=True))
        return (state_out, (gated * lax.rsqrt(mean_square + EPS) * norm_gain).astype(jnp.bfloat16))
    _, mixed_rows = lax.scan(one_row, start, (x_rows, gate_rows, b_rows, c_rows, log_decay, step_size))
    return mixed_rows.reshape(TOKENS, D)
```

```python
import functools

import jax
import jax.numpy as jnp
from jax import lax
from jax.experimental import pallas as pl
from jax.experimental.pallas import tpu as pltpu
from jax.sharding import Mesh
from jax.sharding import PartitionSpec as P

D = 1024
ROW = 512
EPS = 1e-05
SEQ = ("seq_0", "seq_1", "seq_2")
Q = 128
H = 4
W = 64
N = 128
LOG2E = 1.4426950408889634
F32 = jnp.float32
BF16 = jnp.bfloat16


def softplus(x):
    u = jnp.exp(-jnp.abs(x))
    series = u * (1.0 + u * (-1 / 2 + u * (1 / 3 + u * (-1 / 4 + u * (1 / 5 + u * (-1 / 6 + u * (1 / 7)))))))
    return jnp.maximum(x, 0.0) + jnp.where(u < 0.0625, series, jnp.log(1.0 + u))


def exact_dot(a, b):
    hi = a.astype(BF16)
    rest = a - hi.astype(F32)
    mid = rest.astype(BF16)
    low = (rest - mid.astype(F32)).astype(BF16)
    dot = lambda p: jnp.dot(p, b, preferred_element_type=F32)
    return dot(hi) + (dot(mid) + dot(low))


def decay_group(g, group, raw_ref, bias_ref, rate_ref, tissue_ref, tri, cols_ref, rows_ref, sums_ref, total):
    lane = lax.broadcasted_iota(jnp.int32, (H, Q), 1)
    steps = []
    for k in range(group):
        c = g * group + k
        r = c // (ROW // Q)
        raw = raw_ref[:, pl.ds(pl.multiple_of(c * Q, Q), Q)]
        place = lane + (c % (ROW // Q)) * Q
        inside = (place >= tissue_ref[2 * r]) & (place < tissue_ref[2 * r + 1])
        steps.append(jnp.where(inside, softplus(raw + bias_ref[...]), 0.0))
    step = jnp.concatenate(steps, axis=0)
    log2_decay = step * jnp.concatenate([rate_ref[...]] * group, axis=0)
    both = exact_dot(log2_decay, tri)
    run, tot = both[:, :Q], both[:, Q:]
    key = run - jnp.log(step) * LOG2E
    left = jnp.exp2(tot - run) * step
    grown = jnp.exp2(run)
    for k in range(group):
        c = g * group + k
        at = slice(k * H, (k + 1) * H)
        cols_ref[c] = jnp.concatenate([run[at], grown[at]], axis=0)
        rows_ref[c] = jnp.concatenate([key[at], left[at]], axis=0)
        sums_ref[c] = jnp.concatenate([tot[at], total], axis=0)
        total = total + tot[at]
    return total


def triangle():
    i = lax.broadcasted_iota(jnp.int32, (Q, 2 * Q), 0)
    j = lax.broadcasted_iota(jnp.int32, (Q, 2 * Q), 1)
    return jnp.where((i <= j), 1.0, 0.0).astype(BF16)


def per_head_lanes(rows, k):
    lane = lax.broadcasted_iota(jnp.int32, (1, 2 * W), 1)
    pieces = [
        jnp.where(lane < W, rows[k + 2 * p : k + 2 * p + 1], rows[k + 2 * p + 1 : k + 2 * p + 2])
        for p in range(H // 2)
    ]
    return jnp.concatenate(pieces, axis=1)


def split_pair(x, p):
    lane = lax.broadcasted_iota(jnp.int32, (Q, 2 * W), 1)
    pair = x[:, 2 * W * p : 2 * W * (p + 1)]
    zero = jnp.zeros_like(pair)
    return jnp.concatenate([jnp.where(lane < W, pair, zero), jnp.where(lane < W, zero, pair)], axis=0)


def fresh_state(bt, left, pairs):
    b = bt.astype(F32)
    out = []
    for p in range(H // 2):
        scaled = [(b * left[h : h + 1]).astype(BF16) for h in (2 * p, 2 * p + 1)]
        out.append(jnp.dot(jnp.concatenate(scaled, axis=1), pairs[p], preferred_element_type=F32))
    return jnp.concatenate(out, axis=1)


def band_state_chunk(x, bt, rows, sums, total):
    ahead = total - sums[H : 2 * H] - sums[0:H]
    left = rows[H : 2 * H] * jnp.exp2(ahead)
    return fresh_state(bt, left, [split_pair(x, p) for p in range(H // 2)])


def output_chunk(x, gate, bt, ct, cols, rows, sums, skip, state):
    c = ct.T
    pairs = [split_pair(x, p) for p in range(H // 2)]
    scores = jnp.dot(c, bt, preferred_element_type=F32)
    t = lax.broadcasted_iota(jnp.int32, (Q, Q), 0)
    s = lax.broadcasted_iota(jnp.int32, (Q, Q), 1)
    scores = jnp.where(t >= s, scores, 0.0)
    carried = jnp.dot(c, state.astype(BF16), preferred_element_type=F32)
    col = cols.T
    lane = lax.broadcasted_iota(jnp.int32, (Q, 2 * W), 1)
    inner = []
    grown = []
    for p in range(H // 2):
        weights = []
        for h in (2 * p, 2 * p + 1):
            gap = jnp.minimum(col[:, h : h + 1] - rows[h : h + 1], 127.0)
            weights.append((scores * jnp.exp2(gap)).astype(BF16))
        inner.append(jnp.dot(jnp.concatenate(weights, axis=1), pairs[p], preferred_element_type=F32))
        k = H + 2 * p
        grown.append(jnp.where(lane < W, col[:, k : k + 1], col[:, k + 1 : k + 2]))
    inner = jnp.concatenate(inner, axis=1)
    grown = jnp.concatenate(grown, axis=1)
    y = inner + grown * carried + skip * x.astype(F32)
    half = gate.astype(F32) * 0.5
    gated = y * (half + half * jnp.tanh(half))
    square = gated * gated
    square = square[:, :Q] + square[:, Q:]
    squares = jnp.sum(square.T, axis=0, keepdims=True)
    state = jnp.exp2(per_head_lanes(sums, 0)) * state + fresh_state(bt, rows[H : 2 * H], pairs)
    return gated, squares, state


def decay_kernel(group, raw_ref, bias_ref, rate_ref, tissue_ref, cols_ref, rows_ref, sums_ref, total_ref):
    tri = triangle()
    count = cols_ref.shape[0] // group
    step = lambda g, total: decay_group(
        g, group, raw_ref, bias_ref, rate_ref, tissue_ref, tri, cols_ref, rows_ref, sums_ref, total
    )
    total_ref[...] = lax.fori_loop(0, count, step, jnp.zeros((H, Q), F32))


def state_kernel(x_ref, bt_ref, rows_ref, sums_ref, total_ref, state_ref):
    @pl.when(pl.program_id(0) == 0)
    def _():
        state_ref[...] = jnp.zeros_like(state_ref)

    acc = state_ref[...]
    for k in range(ROW // Q):
        acc = acc + band_state_chunk(
            x_ref[k * Q : (k + 1) * Q, :],
            bt_ref[:, k * Q : (k + 1) * Q],
            rows_ref[k],
            sums_ref[k],
            total_ref[...],
        )
    state_ref[...] = acc


def output_kernel(
    x_ref, gate_ref, bt_ref, ct_ref, cols_ref, rows_ref, sums_ref, skip_ref, start_ref, gated_ref, squares_ref, state_ref
):
    @pl.when(pl.program_id(0) == 0)
    def _():
        state_ref[...] = start_ref[...]

    for k in range(ROW // Q):
        at = slice(k * Q, (k + 1) * Q)
        gated, squares, state = output_chunk(
            x_ref[at, :],
            gate_ref[at, :],
            bt_ref[:, at],
            ct_ref[:, at],
            cols_ref[k],
            rows_ref[k],
            sums_ref[k],
            skip_ref[...],
            state_ref[...],
        )
        gated_ref[at, :] = gated
        squares_ref[:, at] = squares
        state_ref[...] = state


def norm_kernel(gated_ref, squares_ref, gain_ref, out_ref):
    block = gated_ref.shape[0]
    mean = jnp.sum(squares_ref[...], axis=0, keepdims=True) / D
    scale = lax.rsqrt(mean + EPS)
    gain = gain_ref[...]
    for k in range(block // Q):
        col = jnp.broadcast_to(scale[:, k * Q : (k + 1) * Q], (8, Q)).T[:, 0:1]
        out_ref[k * Q : (k + 1) * Q, :] = (gated_ref[k * Q : (k + 1) * Q, :] * col * gain).astype(BF16)


def per_device(
    features, gate_input, input_map, output_map, step_raw, step_bias, decay_log, skip_gain, norm_gain, tissue
):
    tokens, width = features.shape
    chunks = tokens // Q
    bt = lax.all_gather(input_map.T, "chan", axis=0, tiled=True)
    ct = lax.all_gather(output_map.T, "chan", axis=0, tiled=True)
    bias = jnp.broadcast_to(step_bias[:, None], (H, Q))
    rate = jnp.broadcast_to((-LOG2E * jnp.exp(decay_log))[:, None], (H, Q))
    skip = jnp.repeat(skip_gain, W)[None, :]
    vmem = pl.BlockSpec(memory_space=pltpu.VMEM)
    per_chunk = jax.ShapeDtypeStruct((chunks, 2 * H, Q), F32)
    cols, rows, sums, total = pl.pallas_call(
        functools.partial(decay_kernel, 8),
        out_shape=(per_chunk, per_chunk, per_chunk, jax.ShapeDtypeStruct((H, Q), F32)),
        in_specs=[vmem, vmem, vmem, pl.BlockSpec(memory_space=pltpu.SMEM)],
        out_specs=(vmem, vmem, vmem, vmem),
        name="decays",
    )(step_raw.T, bias, rate, tissue.reshape(-1))
    k = ROW // Q
    token_block = pl.BlockSpec((ROW, width), lambda i: (i, 0))
    map_block = pl.BlockSpec((N, ROW), lambda i: (0, i))
    chunk_block = pl.BlockSpec((k, 2 * H, Q), lambda i: (i, 0, 0))
    whole = lambda shape: pl.BlockSpec(shape, lambda i: (0, 0))
    state = pl.pallas_call(
        state_kernel,
        grid=(tokens // ROW,),
        out_shape=jax.ShapeDtypeStruct((N, width), F32),
        in_specs=[token_block, map_block, chunk_block, chunk_block, whole((H, Q))],
        out_specs=whole((N, width)),
        name="states",
    )(features, bt, rows, sums, total)
    states = lax.all_gather(state, SEQ)
    totals = lax.all_gather(total[:, 0], SEQ)
    bands = lax.axis_size(SEQ)
    me = lax.axis_index(SEQ)
    order = jnp.arange(bands)
    between = (order[None, :] > order[:, None]) & (order[None, :] < me)
    reach = jnp.sum(jnp.where(between[:, :, None], totals[None], 0.0), axis=1)
    factor = jnp.where((order < me)[:, None], jnp.exp2(reach), 0.0)
    start = jnp.sum(jnp.repeat(factor, W, axis=1)[:, None, :] * states, axis=0)
    gated, squares = pl.pallas_call(
        output_kernel,
        grid=(tokens // ROW,),
        out_shape=(jax.ShapeDtypeStruct((tokens, width), F32), jax.ShapeDtypeStruct((1, tokens), F32)),
        in_specs=[
            token_block,
            token_block,
            map_block,
            map_block,
            chunk_block,
            chunk_block,
            chunk_block,
            whole((1, width)),
            whole((N, width)),
        ],
        out_specs=(token_block, pl.BlockSpec((1, ROW), lambda i: (0, i))),
        scratch_shapes=[pltpu.VMEM((N, width), F32)],
        name="outputs",
    )(features, gate_input, bt, ct, cols, rows, sums, skip, start)
    everyone = lax.all_gather(squares[0], "chan")
    return pl.pallas_call(
        norm_kernel,
        grid=(tokens // (2 * ROW),),
        out_shape=jax.ShapeDtypeStruct((tokens, width), BF16),
        in_specs=[
            pl.BlockSpec((2 * ROW, width), lambda i: (i, 0)),
            pl.BlockSpec((4, 2 * ROW), lambda i: (0, i)),
            whole((1, width)),
        ],
        out_specs=pl.BlockSpec((2 * ROW, width), lambda i: (i, 0)),
        name="norm",
    )(gated, everyone, norm_gain[None, :])


def solution(mesh):
    split = Mesh(mesh.devices.reshape(4, 4, 2, mesh.shape["chan"]), (*SEQ, "chan"))
    tokens = P(SEQ, "chan")
    placed = (tokens,) * 5 + (P("chan"),) * 4 + (P(SEQ, None),)
    return jax.shard_map(per_device, mesh=split, in_specs=placed, out_specs=tokens, check_vma=False)
```

```python
import jax
import jax.numpy as jnp
from jax import lax
from jax.experimental import pallas as pl
from jax.experimental.pallas import tpu as pltpu
from jax.sharding import Mesh
from jax.sharding import PartitionSpec as P

D = 1024
ROW = 512
EPS = 1e-05
SEQ = ("seq_0", "seq_1", "seq_2")
Q = 128
H = 4
W = 64
N = 128
LOG2E = 1.4426950408889634
SEGS = 8
LEAD = 2
BAND = 4
INTRA = 6
FINISH = 6
MESH = pl.DeviceIdType.MESH
F32 = jnp.float32
BF16 = jnp.bfloat16


def softplus(x):
    u = jnp.exp(-jnp.abs(x))
    series = u * (1.0 + u * (-1 / 2 + u * (1 / 3 + u * (-1 / 4 + u * (1 / 5 + u * (-1 / 6 + u * (1 / 7)))))))
    return jnp.maximum(x, 0.0) + jnp.where(u < 0.0625, series, jnp.log(1.0 + u))


def three_parts(a):
    hi = a.astype(BF16)
    rest = a - hi.astype(F32)
    mid = rest.astype(BF16)
    low = (rest - mid.astype(F32)).astype(BF16)
    return hi, mid, low


def exact_dot(a, b):
    hi, mid, low = (jnp.dot(p, b, preferred_element_type=F32) for p in three_parts(a))
    return hi + (mid + low)


def decay_group(g, group, raw_ref, bias, rate, tissue_ref, tri, cols_ref, gaps_ref, rows_ref, sums_ref, total):
    lane = lax.broadcasted_iota(jnp.int32, (H, Q), 1)
    steps = []
    for k in range(group):
        c = g * group + k
        r = c // (ROW // Q)
        raw = raw_ref[:, pl.ds(pl.multiple_of(c * Q, Q), Q)]
        place = lane + (c % (ROW // Q)) * Q
        inside = (place >= tissue_ref[0, r]) & (place < tissue_ref[1, r])
        steps.append(jnp.where(inside, softplus(raw + bias), 0.0))
    step = jnp.concatenate(steps, axis=0)
    log2_decay = step * jnp.concatenate([rate] * group, axis=0)
    both = exact_dot(log2_decay, tri)
    run, tot = both[:, :Q], both[:, Q:]
    key = jnp.minimum(run - jnp.log(step) * LOG2E, 1e30)
    left = jnp.exp2(tot - run) * step
    run_parts, key_parts, grown_parts = (
        [p.astype(F32) for p in three_parts(a)] for a in (run, key, jnp.exp2(run))
    )
    ones = jnp.ones((H, Q), F32)
    row = lax.broadcasted_iota(jnp.int32, (4 * H, Q), 0)
    for k in range(group):
        c = g * group + k
        at = slice(k * H, (k + 1) * H)
        parts = [p[at] for p in run_parts] + [ones] + [p[at] for p in grown_parts] + [jnp.zeros_like(ones)]
        cols_ref[c] = jnp.concatenate(parts, axis=0).astype(BF16)
        for h in range(H):
            block = jnp.where((row < 3 * H) & (row % H == h), 1.0, 0.0)
            for i, p in enumerate(key_parts):
                block = jnp.where(row == 3 * H + i, -p[k * H + h : k * H + h + 1], block)
            gaps_ref[c, :, h * Q : (h + 1) * Q] = block.astype(BF16)
        rows_ref[c] = left[at]
        sums_ref[c] = jnp.concatenate([tot[at], total], axis=0)
        total = total + tot[at]
    return total


def triangle():
    i = lax.broadcasted_iota(jnp.int32, (Q, 2 * Q), 0)
    j = lax.broadcasted_iota(jnp.int32, (Q, 2 * Q), 1)
    return jnp.where((i <= j), 1.0, 0.0).astype(BF16)


def per_head_lanes(rows, k):
    lane = lax.broadcasted_iota(jnp.int32, (1, 2 * W), 1)
    pieces = [
        jnp.where(lane < W, rows[k + 2 * p : k + 2 * p + 1], rows[k + 2 * p + 1 : k + 2 * p + 2])
        for p in range(H // 2)
    ]
    return jnp.concatenate(pieces, axis=1)


def split_pair(x, p):
    lane = lax.broadcasted_iota(jnp.int32, (Q, 2 * W), 1)
    pair = x[:, 2 * W * p : 2 * W * (p + 1)]
    zero = jnp.zeros_like(pair)
    return jnp.concatenate([jnp.where(lane < W, pair, zero), jnp.where(lane < W, zero, pair)], axis=0)


def fresh_state(bt, left, pairs):
    b = bt.astype(F32)
    out = []
    for p in range(H // 2):
        scaled = [(b * left[h : h + 1]).astype(BF16) for h in (2 * p, 2 * p + 1)]
        out.append(jnp.dot(jnp.concatenate(scaled, axis=1), pairs[p], preferred_element_type=F32))
    return jnp.concatenate(out, axis=1)


def row_per_head(values):
    row = lax.broadcasted_iota(jnp.int32, (H, Q), 0)
    out = jnp.full((H, Q), values[0], F32)
    for h in range(1, H):
        out = jnp.where(row == h, values[h], out)
    return out


def join(states, totals, me):
    count = len(states)
    before = before_log = whole = whole_log = 0.0
    reach = jnp.zeros_like(totals[0])
    after = jnp.zeros_like(totals[0])
    for k in reversed(range(count)):
        is_before = k < me
        weight = jnp.where(is_before, jnp.exp2(reach), 0.0)
        before = before + per_head_lanes(weight, 0) * states[k]
        whole = whole + per_head_lanes(jnp.exp2(after), 0) * states[k]
        reach = reach + jnp.where(is_before, totals[k], 0.0)
        after = after + totals[k]
    return (reach, before), (after, whole)


def main_kernel(
    x_hbm,
    gate_hbm,
    b_hbm,
    c_hbm,
    raw_hbm,
    bias_smem,
    decay_smem,
    skip_smem,
    tissue_ref,
    gated_hbm,
    scale_ref,
    raw_ref,
    x_ref,
    gate_ref,
    y_ref,
    silu_ref,
    starts,
    gated_ref,
    maps,
    cols_ref,
    gaps_ref,
    ct_ref,
    rows_ref,
    sums_ref,
    state_ref,
    squares,
    core_s,
    core_l,
    y_s,
    y_l,
    z_s,
    z_l,
    local_sem,
    load_sem,
    gate_sem,
    out_sem,
    map_send,
    map_recv,
    near_send,
    near_recv,
    far_send,
    far_recv,
    sq_send,
    sq_recv,
):
    tokens = x_ref.shape[0]
    chunks = tokens // Q
    per_seg = chunks // SEGS
    seg = tokens // SEGS
    half = maps.shape[3] // 2
    z, yy, core, me = (lax.axis_index(a) for a in (*SEQ, "chan"))
    around = lax.axis_size("chan")
    right, left = lax.rem(me + 1, around), lax.rem(me + around - 1, around)

    def map_load(a, g):
        at = pl.ds(g * seg, seg)
        return pltpu.make_async_copy((b_hbm, c_hbm)[a].at[:, at], maps.at[a, 0, g], load_sem.at[a, g])

    load_x = pltpu.make_async_copy(x_hbm, x_ref, local_sem.at[0])
    load_raw = pltpu.make_async_copy(raw_hbm, raw_ref, local_sem.at[1])

    def gate_load(g):
        at = pl.ds(pl.multiple_of(g * seg, Q), seg)
        return pltpu.make_async_copy(gate_hbm.at[at, :], gate_ref.at[lax.rem(g, 2)], gate_sem.at[g])

    for g in range(SEGS):
        map_load(0, g).start()
    load_raw.start()
    squares[me] = jnp.zeros_like(squares[0])

    barrier = pltpu.get_barrier_semaphore()
    peers = [{"chan": lax.rem(me + d, around)} for d in (1, 2, 3)]
    peers += [{"seq_1": lax.rem(yy + d, 4)} for d in (1, 2, 3)]
    peers += [{"seq_0": lax.rem(z + d, 4)} for d in (1, 2, 3)]
    peers += [{"seq_2": 1 - core}]
    for peer in peers:
        pl.semaphore_signal(barrier, inc=1, device_id=peer, device_id_type=MESH)
    pl.semaphore_wait(barrier, len(peers))

    def remote(src, dst, send, recv, peer):
        return pltpu.make_async_remote_copy(
            src_ref=src, dst_ref=dst, send_sem=send, recv_sem=recv, device_id=peer, device_id_type=MESH
        )

    def map_copy(k, j):
        a, g = j // SEGS, lax.rem(j, SEGS)
        whole, first, second = slice(0, 2 * half), slice(0, half), slice(half, 2 * half)
        plan = (
            (0, 1, whole, right),
            (0, 2, whole, left),
            (1, 3, first, right),
            (2, 3, second, left),
        )
        src, dst, at, peer = plan[k]
        return remote(
            maps.at[a, src, g, at],
            maps.at[a, dst, g, at],
            map_send.at[k, j],
            map_recv.at[k, j],
            {"chan": peer},
        )

    def send_own(j):
        map_copy(0, j).start()
        map_copy(1, j).start()

    def service(j):
        map_copy(0, j).wait_recv()
        map_copy(2, j).start()
        map_copy(1, j).wait_recv()
        map_copy(3, j).start()

        @pl.when(j + LEAD < 2 * SEGS)
        def _():
            send_own(j + LEAD)

    def wait_far(j):
        map_copy(2, j).wait_recv()
        map_copy(3, j).wait_recv()

    for j in range(LEAD):
        map_load(0, j).wait()
        send_own(j)
    for j in range(LEAD, SEGS):
        map_load(0, j).wait()
    for g in range(SEGS):
        map_load(1, g).start()
    load_x.start()
    gate_load(0).start()
    gate_load(1).start()
    load_raw.wait()
    bias = row_per_head([bias_smem[h] for h in range(H)])
    rate = jnp.exp(row_per_head([decay_smem[h] for h in range(H)])) * -LOG2E
    skip = per_head_lanes(row_per_head([skip_smem[h] for h in range(H)]), 0)

    tri = triangle()
    group = 8
    total = lax.fori_loop(
        0,
        chunks // group,
        lambda g, t: decay_group(
            g, group, raw_ref, bias, rate, tissue_ref, tri, cols_ref, gaps_ref, rows_ref, sums_ref, t
        ),
        jnp.zeros((H, Q), F32),
    )
    for g in range(SEGS):
        map_load(1, g).wait()
    load_x.wait()
    state_ref[...] = jnp.zeros_like(state_ref)

    def tokens_of(c):
        return pl.ds(pl.multiple_of(c * Q, Q), Q)

    def map_of(a, c):
        g = c // per_seg
        return maps[a, :, g, :, tokens_of(c - g * per_seg)].reshape(N, Q)

    def band_some(g, i):
        fresh, decay, silu, direct = [], [], [], []
        for k in range(BAND):
            c = g * per_seg + i * BAND + k
            rows = rows_ref[c]
            x = x_ref[tokens_of(c), :]
            pairs = [split_pair(x, p) for p in range(H // 2)]
            fresh.append(fresh_state(map_of(0, c), rows, pairs))
            decay.append(jnp.exp2(per_head_lanes(sums_ref[c], 0)))
            gate = gate_ref[lax.rem(g, 2), tokens_of(i * BAND + k), :].astype(F32) * 0.5
            silu.append(gate + gate * jnp.tanh(gate))
            direct.append(skip * x.astype(F32))
        state = state_ref[...]
        states = []
        for k in range(BAND):
            states.append(state)
            state = decay[k] * state + fresh[k]
        state_ref[...] = state
        for k in range(BAND):
            c = g * per_seg + i * BAND + k
            starts[c] = states[k]
            silu_ref[tokens_of(c), :] = silu[k]
            y_ref[tokens_of(c), :] = direct[k]

    def band_seg(g):
        gate_load(g).wait()
        lax.fori_loop(0, per_seg // BAND, lambda i, carry: (band_some(g, i), carry)[1], 0)

        @pl.when(g + 2 < SEGS)
        def _():
            gate_load(g + 2).start()

    def intra_some(g, i):
        out, turned = [], []
        t = lax.broadcasted_iota(jnp.int32, (Q, Q), 0)
        s = lax.broadcasted_iota(jnp.int32, (Q, Q), 1)
        for k in range(INTRA):
            c = g * per_seg + i * INTRA + k
            x = x_ref[tokens_of(c), :]
            cm = map_of(1, c).T
            turned.append(cm)
            scores = jnp.dot(cm, map_of(0, c), preferred_element_type=F32)
            scores = jnp.where(t >= s, scores, 0.0)
            gap = jnp.dot(cols_ref[c, : 4 * H, :].T, gaps_ref[c], preferred_element_type=F32)
            damp = jnp.exp2(jnp.minimum(gap, 127.0))
            inner = []
            for p in range(H // 2):
                weights = [(scores * damp[:, h * Q : (h + 1) * Q]).astype(BF16) for h in (2 * p, 2 * p + 1)]
                inner.append(
                    jnp.dot(jnp.concatenate(weights, axis=1), split_pair(x, p), preferred_element_type=F32)
                )
            out.append(y_ref[tokens_of(c), :] + jnp.concatenate(inner, axis=1))
        for k in range(INTRA):
            at = tokens_of(g * per_seg + i * INTRA + k)
            y_ref[at, :] = out[k]
            ct_ref[at, :] = turned[k]

    def intra_seg(g):
        lax.fori_loop(0, per_seg // INTRA, lambda i, carry: (intra_some(g, i), carry)[1], 0)

    def finish_some(g, i):
        out, sums_out = [], []
        entering = state_ref[...]
        row = lax.broadcasted_iota(jnp.int32, (4 * H, H * W), 0)
        lane = lax.broadcasted_iota(jnp.int32, (4 * H, H * W), 1)
        spread = jnp.where((row < 3 * H) & (row % H == lane // W), 1.0, 0.0).astype(BF16)
        for k in range(FINISH):
            c = g * per_seg + i * FINISH + k
            at = tokens_of(c)
            state = starts[c] + jnp.exp2(per_head_lanes(sums_ref[c], H)) * entering
            carried = jnp.dot(ct_ref[at, :], state.astype(BF16), preferred_element_type=F32)
            grown = jnp.dot(cols_ref[c, 4 * H :, :].T, spread, preferred_element_type=F32)
            gated = (y_ref[at, :] + grown * carried) * silu_ref[at, :]
            out.append(gated.astype(BF16))
            square = gated * gated
            square = square[:, :Q] + square[:, Q:]
            sums_out.append(jnp.sum(square.T, axis=0, keepdims=True))
        for k in range(FINISH):
            gated_ref[lax.rem(g, 2), tokens_of(i * FINISH + k), :] = out[k]
            squares[me, g, pl.ds(i * FINISH + k, 1), :] = sums_out[k]

    def gated_copy(g):
        at = pl.ds(pl.multiple_of(g * seg, Q), seg)
        return pltpu.make_async_copy(gated_ref.at[lax.rem(g, 2)], gated_hbm.at[at, :], out_sem.at[g])

    def square_copies(g):
        return [
            remote(
                squares.at[me, g],
                squares.at[me, g],
                sq_send.at[d - 1, g],
                sq_recv.at[d - 1, g],
                {"chan": lax.rem(me + d, around)},
            )
            for d in (1, 2, 3)
        ]

    def finish_seg(g):
        @pl.when(g >= 2)
        def _():
            gated_copy(g - 2).wait()

        lax.fori_loop(0, per_seg // FINISH, lambda i, carry: (finish_some(g, i), carry)[1], 0)
        gated_copy(g).start()
        for copy in square_copies(g):
            copy.start()

    def exchange(slots_s, slots_l, sends, recvs, axis, at):
        size = slots_s.shape[0]
        copies = []
        for d in range(1, size):
            peer = {axis: lax.rem(at + d, size)}
            copies.append(remote(slots_s.at[at], slots_s.at[at], sends(d, 0), recvs(d, 0), peer))
            copies.append(remote(slots_l.at[at], slots_l.at[at], sends(d, 1), recvs(d, 1), peer))
        return copies

    def put(slots_s, slots_l, at, pair):
        slots_l[at] = pair[0]
        slots_s[at] = pair[1].astype(slots_s.dtype)

    def get(slots_s, slots_l, at):
        size = slots_s.shape[0]
        return join([slots_s[k].astype(F32) for k in range(size)], [slots_l[k] for k in range(size)], at)

    service(0)

    def band_step(j, carry):
        service(j)
        wait_far(j - 1)
        band_seg(j - 1)
        return carry

    lax.fori_loop(1, SEGS + 1, band_step, 0)

    near = exchange(core_s, core_l, lambda d, k: near_send.at[k], lambda d, k: near_recv.at[k], "seq_2", core)
    along_y = exchange(
        y_s, y_l, lambda d, k: far_send.at[0, d - 1, k], lambda d, k: far_recv.at[0, d - 1, k], "seq_1", yy
    )
    along_z = exchange(
        z_s, z_l, lambda d, k: far_send.at[1, d - 1, k], lambda d, k: far_recv.at[1, d - 1, k], "seq_0", z
    )

    def inner_step(g, carry=0):
        service(SEGS + g + 1)
        wait_far(SEGS + g)
        intra_seg(g)
        return carry

    def finish_step(g, carry=0):
        finish_seg(g)
        return carry

    put(core_s, core_l, core, (total, state_ref[...]))
    for copy in near:
        copy.start()
    inner_step(0)
    for copy in near:
        copy.wait()
    in_core, chip = get(core_s, core_l, core)
    put(y_s, y_l, yy, chip)
    for copy in along_y:
        copy.start()
    lax.fori_loop(1, 3, inner_step, 0)
    for copy in along_y:
        copy.wait()
    in_y, plane = get(y_s, y_l, yy)
    put(z_s, z_l, z, plane)
    for copy in along_z:
        copy.start()
    lax.fori_loop(3, 5, inner_step, 0)
    for copy in along_z:
        copy.wait()
    in_z, _ = get(z_s, z_l, z)
    lanes = lambda log: per_head_lanes(jnp.exp2(log), 0)
    state_ref[...] = lanes(in_core[0]) * (lanes(in_y[0]) * in_z[1] + in_y[1]) + in_core[1]

    finish_seg(0)
    inner_step(5)
    lax.fori_loop(1, 3, finish_step, 0)
    inner_step(6)
    lax.fori_loop(3, 7, finish_step, 0)
    wait_far(2 * SEGS - 1)
    intra_seg(SEGS - 1)
    finish_seg(SEGS - 1)

    def close(g, carry):
        for copy in square_copies(g):
            copy.wait()
        mean = (squares[0, g] + squares[1, g] + squares[2, g] + squares[3, g]) / D
        scale_ref[g] = lax.rsqrt(mean + EPS)
        return carry

    lax.fori_loop(0, SEGS, close, 0)
    gated_copy(SEGS - 2).wait()
    gated_copy(SEGS - 1).wait()

    def drain(j, carry):
        for k in range(4):
            map_copy(k, j).wait_send()
        return carry

    lax.fori_loop(0, 2 * SEGS, drain, 0)


def norm_kernel(gated_hbm, scale_ref, gain_ref, out_hbm, gated_ref, out_ref, load_sem, store_sem):
    seg = gated_ref.shape[0] // SEGS

    def load(g):
        at = pl.ds(g * seg, seg)
        return pltpu.make_async_copy(gated_hbm.at[at, :], gated_ref.at[at, :], load_sem.at[g])

    def store(g):
        at = pl.ds(g * seg, seg)
        return pltpu.make_async_copy(out_ref.at[at, :], out_hbm.at[at, :], store_sem.at[g])

    for g in range(SEGS):
        load(g).start()

    def one(g, carry):
        col = scale_ref[g].T
        load(g).wait()
        for k in range(seg // Q):
            at = pl.ds(pl.multiple_of(g * seg + k * Q, Q), Q)
            out_ref[at, :] = (gated_ref[at, :].astype(F32) * col[:, k : k + 1] * gain_ref[...]).astype(BF16)
        store(g).start()
        return carry

    lax.fori_loop(0, SEGS, one, 0)
    for g in range(SEGS):
        store(g).wait()


def per_device(
    features, gate_input, input_map, output_map, step_raw, step_bias, decay_log, skip_gain, norm_gain, tissue
):
    tokens, width = features.shape
    chunks = tokens // Q
    vmem = pl.BlockSpec(memory_space=pltpu.VMEM)
    hbm = pl.BlockSpec(memory_space=pl.ANY)
    around = lax.axis_size("chan")
    dma = pltpu.SemaphoreType.DMA
    slots = lambda n, dtype: [pltpu.VMEM((n, N, width), dtype), pltpu.VMEM((n, H, Q), F32)]
    gated, scale = pl.pallas_call(
        main_kernel,
        out_shape=(
            jax.ShapeDtypeStruct((tokens, width), BF16),
            jax.ShapeDtypeStruct((SEGS, 16, Q), F32),
        ),
        in_specs=[hbm] * 5 + [pl.BlockSpec(memory_space=pltpu.SMEM)] * 4,
        out_specs=(hbm, vmem),
        scratch_shapes=[
            pltpu.VMEM((H, tokens), F32),
            pltpu.VMEM((tokens, width), BF16),
            pltpu.VMEM((2, tokens // SEGS, width), BF16),
            pltpu.VMEM((tokens, width), F32),
            pltpu.VMEM((tokens, width), F32),
            pltpu.VMEM((chunks, N, width), F32),
            pltpu.VMEM((2, tokens // SEGS, width), BF16),
            pltpu.VMEM((2, around, SEGS, N // around, tokens // SEGS), BF16),
            pltpu.VMEM((chunks, 8 * H, Q), BF16),
            pltpu.VMEM((chunks, 4 * H, H * Q), BF16),
            pltpu.VMEM((tokens, N), BF16),
            pltpu.VMEM((chunks, H, Q), F32),
            pltpu.VMEM((chunks, 2 * H, Q), F32),
            pltpu.VMEM((N, width), F32),
            pltpu.VMEM((around, SEGS, 16, Q), F32),
            *slots(2, F32),
            *slots(4, BF16),
            *slots(4, BF16),
            dma((2,)),
            dma((2, SEGS)),
            dma((SEGS,)),
            dma((SEGS,)),
            dma((4, 2 * SEGS)),
            dma((4, 2 * SEGS)),
            dma((2,)),
            dma((2,)),
            dma((2, 3, 2)),
            dma((2, 3, 2)),
            dma((3, SEGS)),
            dma((3, SEGS)),
        ],
        compiler_params=pltpu.CompilerParams(
            collective_id=0, has_side_effects=True, vmem_limit_bytes=67043328
        ),
        name="scan",
    )(features, gate_input, input_map.T, output_map.T, step_raw.T, step_bias, decay_log, skip_gain, tissue.T)
    return pl.pallas_call(
        norm_kernel,
        out_shape=jax.ShapeDtypeStruct((tokens, width), BF16),
        in_specs=[hbm, vmem, vmem],
        out_specs=hbm,
        scratch_shapes=[
            pltpu.VMEM((tokens, width), BF16),
            pltpu.VMEM((tokens, width), BF16),
            dma((SEGS,)),
            dma((SEGS,)),
        ],
        compiler_params=pltpu.CompilerParams(vmem_limit_bytes=63 * 1024 * 1024),
        name="norm",
    )(gated, scale, norm_gain[None, :])


def solution(mesh):
    split = Mesh(mesh.devices.reshape(4, 4, 2, mesh.shape["chan"]), (*SEQ, "chan"))
    tokens = P(SEQ, "chan")
    placed = (tokens,) * 5 + (P("chan"),) * 4 + (P(SEQ, None),)
    return jax.shard_map(per_device, mesh=split, in_specs=placed, out_specs=tokens, check_vma=False)
```

```python
import jax
import jax.numpy as jnp
from jax import lax
from jax.experimental import pallas as pl
from jax.experimental.pallas import tpu as pltpu
from jax.sharding import Mesh
from jax.sharding import PartitionSpec as P

D = 1024
ROW = 512
EPS = 1e-05
SEQ = ("seq_0", "seq_1", "seq_2")
Q = 128
H = 4
W = 64
N = 128
LOG2E = 1.4426950408889634
SEGS = 8
LEAD = 2
BAND = 4
INTRA = 6
FINISH = 6
MESH = pl.DeviceIdType.MESH
F32 = jnp.float32
BF16 = jnp.bfloat16


def softplus(x):
    u = jnp.exp(-jnp.abs(x))
    series = u * (1.0 + u * (-1 / 2 + u * (1 / 3 + u * (-1 / 4 + u * (1 / 5 + u * (-1 / 6 + u * (1 / 7)))))))
    return jnp.maximum(x, 0.0) + jnp.where(u < 0.0625, series, jnp.log(1.0 + u))


def three_parts(a):
    hi = a.astype(BF16)
    rest = a - hi.astype(F32)
    mid = rest.astype(BF16)
    low = (rest - mid.astype(F32)).astype(BF16)
    return hi, mid, low


def exact_dot(a, b):
    hi, mid, low = (jnp.dot(p, b, preferred_element_type=F32) for p in three_parts(a))
    return hi + (mid + low)


def decay_group(g, group, raw_ref, bias, rate, tissue_ref, tri, cols_ref, gaps_ref, rows_ref, sums_ref, total):
    lane = lax.broadcasted_iota(jnp.int32, (H, Q), 1)
    steps = []
    for k in range(group):
        c = g * group + k
        r = c // (ROW // Q)
        raw = raw_ref[:, pl.ds(pl.multiple_of(c * Q, Q), Q)]
        place = lane + (c % (ROW // Q)) * Q
        inside = (place >= tissue_ref[0, r]) & (place < tissue_ref[1, r])
        steps.append(jnp.where(inside, softplus(raw + bias), 0.0))
    step = jnp.concatenate(steps, axis=0)
    log2_decay = step * jnp.concatenate([rate] * group, axis=0)
    both = exact_dot(log2_decay, tri)
    run, tot = both[:, :Q], both[:, Q:]
    key = jnp.minimum(run - jnp.log(step) * LOG2E, 1e30)
    left = jnp.exp2(tot - run) * step
    run_parts, key_parts, grown_parts = (
        [p.astype(F32) for p in three_parts(a)] for a in (run, key, jnp.exp2(run))
    )
    ones = jnp.ones((H, Q), F32)
    row = lax.broadcasted_iota(jnp.int32, (4 * H, Q), 0)
    for k in range(group):
        c = g * group + k
        at = slice(k * H, (k + 1) * H)
        parts = [p[at] for p in run_parts] + [ones] + [p[at] for p in grown_parts] + [jnp.zeros_like(ones)]
        cols_ref[c] = jnp.concatenate(parts, axis=0).astype(BF16)
        for h in range(H):
            block = jnp.where((row < 3 * H) & (row % H == h), 1.0, 0.0)
            for i, p in enumerate(key_parts):
                block = jnp.where(row == 3 * H + i, -p[k * H + h : k * H + h + 1], block)
            gaps_ref[c, :, h * Q : (h + 1) * Q] = block.astype(BF16)
        rows_ref[c] = left[at]
        sums_ref[c] = jnp.concatenate([tot[at], total], axis=0)
        total = total + tot[at]
    return total


def triangle():
    i = lax.broadcasted_iota(jnp.int32, (Q, 2 * Q), 0)
    j = lax.broadcasted_iota(jnp.int32, (Q, 2 * Q), 1)
    return jnp.where((i <= j), 1.0, 0.0).astype(BF16)


def per_head_lanes(rows, k):
    lane = lax.broadcasted_iota(jnp.int32, (1, 2 * W), 1)
    pieces = [
        jnp.where(lane < W, rows[k + 2 * p : k + 2 * p + 1], rows[k + 2 * p + 1 : k + 2 * p + 2])
        for p in range(H // 2)
    ]
    return jnp.concatenate(pieces, axis=1)


def split_pair(x, p):
    lane = lax.broadcasted_iota(jnp.int32, (Q, 2 * W), 1)
    pair = x[:, 2 * W * p : 2 * W * (p + 1)]
    zero = jnp.zeros_like(pair)
    return jnp.concatenate([jnp.where(lane < W, pair, zero), jnp.where(lane < W, zero, pair)], axis=0)


def fresh_state(bt, left, pairs):
    b = bt.astype(F32)
    out = []
    for p in range(H // 2):
        scaled = [(b * left[h : h + 1]).astype(BF16) for h in (2 * p, 2 * p + 1)]
        out.append(jnp.dot(jnp.concatenate(scaled, axis=1), pairs[p], preferred_element_type=F32))
    return jnp.concatenate(out, axis=1)


def row_per_head(values):
    row = lax.broadcasted_iota(jnp.int32, (H, Q), 0)
    out = jnp.full((H, Q), values[0], F32)
    for h in range(1, H):
        out = jnp.where(row == h, values[h], out)
    return out


def join(states, totals, me):
    count = len(states)
    before = before_log = whole = whole_log = 0.0
    reach = jnp.zeros_like(totals[0])
    after = jnp.zeros_like(totals[0])
    for k in reversed(range(count)):
        is_before = k < me
        weight = jnp.where(is_before, jnp.exp2(reach), 0.0)
        before = before + per_head_lanes(weight, 0) * states[k]
        whole = whole + per_head_lanes(jnp.exp2(after), 0) * states[k]
        reach = reach + jnp.where(is_before, totals[k], 0.0)
        after = after + totals[k]
    return (reach, before), (after, whole)


def main_kernel(
    x_hbm,
    gate_hbm,
    b_hbm,
    c_hbm,
    raw_hbm,
    bias_smem,
    decay_smem,
    skip_smem,
    tissue_ref,
    gated_hbm,
    scale_ref,
    raw_ref,
    x_ref,
    gate_ref,
    y_ref,
    silu_ref,
    starts,
    gated_ref,
    maps,
    cols_ref,
    gaps_ref,
    ct_ref,
    rows_ref,
    sums_ref,
    state_ref,
    squares,
    core_s,
    core_l,
    y_s,
    y_l,
    z_s,
    z_l,
    local_sem,
    load_sem,
    gate_sem,
    out_sem,
    map_send,
    map_recv,
    near_send,
    near_recv,
    far_send,
    far_recv,
    sq_send,
    sq_recv,
):
    tokens = x_ref.shape[0]
    chunks = tokens // Q
    per_seg = chunks // SEGS
    seg = tokens // SEGS
    z, yy, core, me = (lax.axis_index(a) for a in (*SEQ, "chan"))
    around = lax.axis_size("chan")

    def map_load(a, g):
        at = pl.ds(g * seg, seg)
        return pltpu.make_async_copy((b_hbm, c_hbm)[a].at[:, at], maps.at[a, 0, g], load_sem.at[a, g])

    load_x = pltpu.make_async_copy(x_hbm, x_ref, local_sem.at[0])
    load_raw = pltpu.make_async_copy(raw_hbm, raw_ref, local_sem.at[1])

    def gate_load(g):
        at = pl.ds(pl.multiple_of(g * seg, Q), seg)
        return pltpu.make_async_copy(gate_hbm.at[at, :], gate_ref.at[lax.rem(g, 2)], gate_sem.at[g])

    for g in range(SEGS):
        map_load(0, g).start()
    load_raw.start()
    squares[me] = jnp.zeros_like(squares[0])

    barrier = pltpu.get_barrier_semaphore()
    peers = [{"chan": lax.rem(me + d, around)} for d in (1, 2, 3)]
    peers += [{"seq_1": lax.rem(yy + d, 4)} for d in (1, 2, 3)]
    peers += [{"seq_0": lax.rem(z + d, 4)} for d in (1, 2, 3)]
    peers += [{"seq_2": 1 - core}]
    for peer in peers:
        pl.semaphore_signal(barrier, inc=1, device_id=peer, device_id_type=MESH)
    pl.semaphore_wait(barrier, len(peers))

    def remote(src, dst, send, recv, peer):
        return pltpu.make_async_remote_copy(
            src_ref=src, dst_ref=dst, send_sem=send, recv_sem=recv, device_id=peer, device_id_type=MESH
        )

    def own_copy(side, j):
        a, g = j // SEGS, lax.rem(j, SEGS)
        peer = {"chan": lax.rem(me + 1 + 2 * side, around)}
        return remote(
            maps.at[a, 0, g], maps.at[a, 1 + side, g], map_send.at[side, j], map_recv.at[side, j], peer
        )

    def far_copy(j):
        a, g, side = j // SEGS, lax.rem(j, SEGS), lax.rem(j, 2)
        peer = {"chan": lax.rem(me + 1 + 2 * side, around)}
        return remote(maps.at[a, 1 + side, g], maps.at[a, 3, g], map_send.at[2, j], map_recv.at[2, j], peer)

    def send_own(j):
        own_copy(0, j).start()
        own_copy(1, j).start()

    def service(j):
        side = lax.rem(j, 2)
        own_copy(side, j).wait_recv()
        far_copy(j).start()
        own_copy(1 - side, j).wait_recv()

        @pl.when(j + LEAD < 2 * SEGS)
        def _():
            send_own(j + LEAD)

    def wait_far(j):
        far_copy(j).wait_recv()

    for j in range(LEAD):
        map_load(0, j).wait()
        send_own(j)
    for j in range(LEAD, SEGS):
        map_load(0, j).wait()
    for g in range(SEGS):
        map_load(1, g).start()
    load_x.start()
    gate_load(0).start()
    gate_load(1).start()
    load_raw.wait()
    bias = row_per_head([bias_smem[h] for h in range(H)])
    rate = jnp.exp(row_per_head([decay_smem[h] for h in range(H)])) * -LOG2E
    skip = per_head_lanes(row_per_head([skip_smem[h] for h in range(H)]), 0)

    tri = triangle()
    group = 8
    total = lax.fori_loop(
        0,
        chunks // group,
        lambda g, t: decay_group(
            g, group, raw_ref, bias, rate, tissue_ref, tri, cols_ref, gaps_ref, rows_ref, sums_ref, t
        ),
        jnp.zeros((H, Q), F32),
    )
    for g in range(SEGS):
        map_load(1, g).wait()
    load_x.wait()
    state_ref[...] = jnp.zeros_like(state_ref)

    def tokens_of(c):
        return pl.ds(pl.multiple_of(c * Q, Q), Q)

    def map_of(a, c):
        g = c // per_seg
        return maps[a, :, g, :, tokens_of(c - g * per_seg)].reshape(N, Q)

    def band_some(g, i):
        fresh, decay, silu, direct = [], [], [], []
        for k in range(BAND):
            c = g * per_seg + i * BAND + k
            rows = rows_ref[c]
            x = x_ref[tokens_of(c), :]
            pairs = [split_pair(x, p) for p in range(H // 2)]
            fresh.append(fresh_state(map_of(0, c), rows, pairs))
            decay.append(jnp.exp2(per_head_lanes(sums_ref[c], 0)))
            gate = gate_ref[lax.rem(g, 2), tokens_of(i * BAND + k), :].astype(F32) * 0.5
            silu.append(gate + gate * jnp.tanh(gate))
            direct.append(skip * x.astype(F32))
        state = state_ref[...]
        states = []
        for k in range(BAND):
            states.append(state)
            state = decay[k] * state + fresh[k]
        state_ref[...] = state
        for k in range(BAND):
            c = g * per_seg + i * BAND + k
            starts[c] = states[k]
            silu_ref[tokens_of(c), :] = silu[k]
            y_ref[tokens_of(c), :] = direct[k]

    def band_seg(g):
        gate_load(g).wait()
        lax.fori_loop(0, per_seg // BAND, lambda i, carry: (band_some(g, i), carry)[1], 0)

        @pl.when(g + 2 < SEGS)
        def _():
            gate_load(g + 2).start()

    def intra_some(g, i):
        t = lax.broadcasted_iota(jnp.int32, (Q, Q), 0)
        s = lax.broadcasted_iota(jnp.int32, (Q, Q), 1)
        def ahead(k):
            c = g * per_seg + i * INTRA + k
            cm = map_of(1, c).T
            gap = jnp.dot(cols_ref[c, : 4 * H, :].T, gaps_ref[c], preferred_element_type=F32)
            scores = jnp.dot(cm, map_of(0, c), preferred_element_type=F32)
            return cm, scores, gap

        coming = [ahead(0), ahead(1)]
        for k in range(INTRA):
            c = g * per_seg + i * INTRA + k
            if k + 2 < INTRA:
                coming.append(ahead(k + 2))
            cm, scores, gap = coming[k]
            ct_ref[tokens_of(c), :] = cm
            x = x_ref[tokens_of(c), :]
            scores = jnp.where(t >= s, scores, 0.0)
            inner = []
            for p in range(H // 2):
                damp = jnp.exp2(jnp.minimum(gap[:, 2 * p * Q : 2 * (p + 1) * Q], 127.0))
                weights = [(scores * damp[:, h * Q : (h + 1) * Q]).astype(BF16) for h in range(2)]
                inner.append(
                    jnp.dot(jnp.concatenate(weights, axis=1), split_pair(x, p), preferred_element_type=F32)
                )
            y_ref[tokens_of(c), :] += jnp.concatenate(inner, axis=1)

    def intra_seg(g):
        lax.fori_loop(0, per_seg // INTRA, lambda i, carry: (intra_some(g, i), carry)[1], 0)

    def finish_some(g, i):
        out, sums_out = [], []
        entering = state_ref[...]
        row = lax.broadcasted_iota(jnp.int32, (4 * H, H * W), 0)
        lane = lax.broadcasted_iota(jnp.int32, (4 * H, H * W), 1)
        spread = jnp.where((row < 3 * H) & (row % H == lane // W), 1.0, 0.0).astype(BF16)
        for k in range(FINISH):
            c = g * per_seg + i * FINISH + k
            at = tokens_of(c)
            state = starts[c] + jnp.exp2(per_head_lanes(sums_ref[c], H)) * entering
            carried = jnp.dot(ct_ref[at, :], state.astype(BF16), preferred_element_type=F32)
            grown = jnp.dot(cols_ref[c, 4 * H :, :].T, spread, preferred_element_type=F32)
            gated = (y_ref[at, :] + grown * carried) * silu_ref[at, :]
            out.append(gated.astype(BF16))
            square = gated * gated
            square = square[:, :Q] + square[:, Q:]
            sums_out.append(jnp.sum(square.T, axis=0, keepdims=True))
        for k in range(FINISH):
            gated_ref[lax.rem(g, 2), tokens_of(i * FINISH + k), :] = out[k]
            squares[me, g, pl.ds(i * FINISH + k, 1), :] = sums_out[k]

    def gated_copy(g):
        at = pl.ds(pl.multiple_of(g * seg, Q), seg)
        return pltpu.make_async_copy(gated_ref.at[lax.rem(g, 2)], gated_hbm.at[at, :], out_sem.at[g])

    def square_copies(g):
        return [
            remote(
                squares.at[me, g],
                squares.at[me, g],
                sq_send.at[d - 1, g],
                sq_recv.at[d - 1, g],
                {"chan": lax.rem(me + d, around)},
            )
            for d in (1, 2, 3)
        ]

    def finish_seg(g):
        @pl.when(g >= 2)
        def _():
            gated_copy(g - 2).wait()

        lax.fori_loop(0, per_seg // FINISH, lambda i, carry: (finish_some(g, i), carry)[1], 0)
        gated_copy(g).start()
        for copy in square_copies(g):
            copy.start()

    def exchange(slots_s, slots_l, sends, recvs, axis, at):
        size = slots_s.shape[0]
        copies = []
        for d in range(1, size):
            peer = {axis: lax.rem(at + d, size)}
            copies.append(remote(slots_s.at[at], slots_s.at[at], sends(d, 0), recvs(d, 0), peer))
            copies.append(remote(slots_l.at[at], slots_l.at[at], sends(d, 1), recvs(d, 1), peer))
        return copies

    def put(slots_s, slots_l, at, pair):
        slots_l[at] = pair[0]
        slots_s[at] = pair[1].astype(slots_s.dtype)

    def get(slots_s, slots_l, at):
        size = slots_s.shape[0]
        return join([slots_s[k].astype(F32) for k in range(size)], [slots_l[k] for k in range(size)], at)

    service(0)

    def band_step(j, carry):
        service(j)
        wait_far(j - 1)
        band_seg(j - 1)
        return carry

    lax.fori_loop(1, SEGS + 1, band_step, 0)

    near = exchange(core_s, core_l, lambda d, k: near_send.at[k], lambda d, k: near_recv.at[k], "seq_2", core)
    along_y = exchange(
        y_s, y_l, lambda d, k: far_send.at[0, d - 1, k], lambda d, k: far_recv.at[0, d - 1, k], "seq_1", yy
    )
    along_z = exchange(
        z_s, z_l, lambda d, k: far_send.at[1, d - 1, k], lambda d, k: far_recv.at[1, d - 1, k], "seq_0", z
    )

    def inner_step(g, carry=0):
        service(SEGS + g + 1)
        wait_far(SEGS + g)
        intra_seg(g)
        return carry

    def finish_step(g, carry=0):
        finish_seg(g)
        return carry

    put(core_s, core_l, core, (total, state_ref[...]))
    for copy in near:
        copy.start()
    inner_step(0)
    for copy in near:
        copy.wait()
    in_core, chip = get(core_s, core_l, core)
    put(y_s, y_l, yy, chip)
    for copy in along_y:
        copy.start()
    lax.fori_loop(1, 3, inner_step, 0)
    for copy in along_y:
        copy.wait()
    in_y, plane = get(y_s, y_l, yy)
    put(z_s, z_l, z, plane)
    for copy in along_z:
        copy.start()
    lax.fori_loop(3, 5, inner_step, 0)
    for copy in along_z:
        copy.wait()
    in_z, _ = get(z_s, z_l, z)
    lanes = lambda log: per_head_lanes(jnp.exp2(log), 0)
    state_ref[...] = lanes(in_core[0]) * (lanes(in_y[0]) * in_z[1] + in_y[1]) + in_core[1]

    finish_seg(0)
    inner_step(5)
    lax.fori_loop(1, 3, finish_step, 0)
    inner_step(6)
    lax.fori_loop(3, 7, finish_step, 0)
    wait_far(2 * SEGS - 1)
    intra_seg(SEGS - 1)
    finish_seg(SEGS - 1)

    def close(g, carry):
        for copy in square_copies(g):
            copy.wait()
        mean = (squares[0, g] + squares[1, g] + squares[2, g] + squares[3, g]) / D
        scale_ref[g] = lax.rsqrt(mean + EPS)
        return carry

    lax.fori_loop(0, SEGS, close, 0)
    gated_copy(SEGS - 2).wait()
    gated_copy(SEGS - 1).wait()

    def drain(j, carry):
        own_copy(0, j).wait_send()
        own_copy(1, j).wait_send()
        far_copy(j).wait_send()
        return carry

    lax.fori_loop(0, 2 * SEGS, drain, 0)


def norm_kernel(gated_hbm, scale_ref, gain_ref, out_hbm, gated_ref, out_ref, load_sem, store_sem):
    seg = gated_ref.shape[0] // SEGS

    def load(g):
        at = pl.ds(g * seg, seg)
        return pltpu.make_async_copy(gated_hbm.at[at, :], gated_ref.at[at, :], load_sem.at[g])

    def store(g):
        at = pl.ds(g * seg, seg)
        return pltpu.make_async_copy(out_ref.at[at, :], out_hbm.at[at, :], store_sem.at[g])

    for g in range(SEGS):
        load(g).start()

    def one(g, carry):
        col = scale_ref[g].T
        load(g).wait()
        for k in range(seg // Q):
            at = pl.ds(pl.multiple_of(g * seg + k * Q, Q), Q)
            out_ref[at, :] = (gated_ref[at, :].astype(F32) * col[:, k : k + 1] * gain_ref[...]).astype(BF16)
        store(g).start()
        return carry

    lax.fori_loop(0, SEGS, one, 0)
    for g in range(SEGS):
        store(g).wait()


def per_device(
    features, gate_input, input_map, output_map, step_raw, step_bias, decay_log, skip_gain, norm_gain, tissue
):
    tokens, width = features.shape
    chunks = tokens // Q
    vmem = pl.BlockSpec(memory_space=pltpu.VMEM)
    hbm = pl.BlockSpec(memory_space=pl.ANY)
    around = lax.axis_size("chan")
    dma = pltpu.SemaphoreType.DMA
    slots = lambda n, dtype: [pltpu.VMEM((n, N, width), dtype), pltpu.VMEM((n, H, Q), F32)]
    gated, scale = pl.pallas_call(
        main_kernel,
        out_shape=(
            jax.ShapeDtypeStruct((tokens, width), BF16),
            jax.ShapeDtypeStruct((SEGS, 16, Q), F32),
        ),
        in_specs=[hbm] * 5 + [pl.BlockSpec(memory_space=pltpu.SMEM)] * 4,
        out_specs=(hbm, vmem),
        scratch_shapes=[
            pltpu.VMEM((H, tokens), F32),
            pltpu.VMEM((tokens, width), BF16),
            pltpu.VMEM((2, tokens // SEGS, width), BF16),
            pltpu.VMEM((tokens, width), F32),
            pltpu.VMEM((tokens, width), F32),
            pltpu.VMEM((chunks, N, width), F32),
            pltpu.VMEM((2, tokens // SEGS, width), BF16),
            pltpu.VMEM((2, around, SEGS, N // around, tokens // SEGS), BF16),
            pltpu.VMEM((chunks, 8 * H, Q), BF16),
            pltpu.VMEM((chunks, 4 * H, H * Q), BF16),
            pltpu.VMEM((tokens, N), BF16),
            pltpu.VMEM((chunks, H, Q), F32),
            pltpu.VMEM((chunks, 2 * H, Q), F32),
            pltpu.VMEM((N, width), F32),
            pltpu.VMEM((around, SEGS, 16, Q), F32),
            *slots(2, F32),
            *slots(4, BF16),
            *slots(4, BF16),
            dma((2,)),
            dma((2, SEGS)),
            dma((SEGS,)),
            dma((SEGS,)),
            dma((3, 2 * SEGS)),
            dma((3, 2 * SEGS)),
            dma((2,)),
            dma((2,)),
            dma((2, 3, 2)),
            dma((2, 3, 2)),
            dma((3, SEGS)),
            dma((3, SEGS)),
        ],
        compiler_params=pltpu.CompilerParams(
            collective_id=0, has_side_effects=True, vmem_limit_bytes=67043328
        ),
        name="scan",
    )(features, gate_input, input_map.T, output_map.T, step_raw.T, step_bias, decay_log, skip_gain, tissue.T)
    return pl.pallas_call(
        norm_kernel,
        out_shape=jax.ShapeDtypeStruct((tokens, width), BF16),
        in_specs=[hbm, vmem, vmem],
        out_specs=hbm,
        scratch_shapes=[
            pltpu.VMEM((tokens, width), BF16),
            pltpu.VMEM((tokens, width), BF16),
            dma((SEGS,)),
            dma((SEGS,)),
        ],
        compiler_params=pltpu.CompilerParams(vmem_limit_bytes=63 * 1024 * 1024),
        name="norm",
    )(gated, scale, norm_gain[None, :])


def solution(mesh):
    split = Mesh(mesh.devices.reshape(4, 4, 2, mesh.shape["chan"]), (*SEQ, "chan"))
    tokens = P(SEQ, "chan")
    placed = (tokens,) * 5 + (P("chan"),) * 4 + (P(SEQ, None),)
    return jax.shard_map(per_device, mesh=split, in_specs=placed, out_specs=tokens, check_vma=False)
```

```python
import jax
import jax.numpy as jnp
from jax import lax
from jax.experimental import pallas as pl
from jax.experimental.pallas import tpu as pltpu
from jax.sharding import Mesh
from jax.sharding import PartitionSpec as P

D = 1024
ROW = 512
EPS = 1e-05
SEQ = ("seq_0", "seq_1", "seq_2")
Q = 128
H = 4
W = 64
N = 128
LOG2E = 1.4426950408889634
SEGS = 8
LEAD = 2
BAND = 4
INTRA = 12
FINISH = 12
MESH = pl.DeviceIdType.MESH
F32 = jnp.float32
BF16 = jnp.bfloat16


def softplus(x):
    u = jnp.exp(-jnp.abs(x))
    series = u * (1.0 + u * (-1 / 2 + u * (1 / 3 + u * (-1 / 4 + u * (1 / 5 + u * (-1 / 6 + u * (1 / 7)))))))
    return jnp.maximum(x, 0.0) + jnp.where(u < 0.0625, series, jnp.log(1.0 + u))


def three_parts(a):
    hi = a.astype(BF16)
    rest = a - hi.astype(F32)
    mid = rest.astype(BF16)
    low = (rest - mid.astype(F32)).astype(BF16)
    return hi, mid, low


def exact_dot(a, b):
    hi, mid, low = (jnp.dot(p, b, preferred_element_type=F32) for p in three_parts(a))
    return hi + (mid + low)


def decay_group(g, group, raw_ref, bias, rate, tissue_ref, tri, cols_ref, gaps_ref, rows_ref, sums_ref, total):
    lane = lax.broadcasted_iota(jnp.int32, (H, Q), 1)
    steps = []
    for k in range(group):
        c = g * group + k
        r = c // (ROW // Q)
        raw = raw_ref[:, pl.ds(pl.multiple_of(c * Q, Q), Q)]
        place = lane + (c % (ROW // Q)) * Q
        inside = (place >= tissue_ref[0, r]) & (place < tissue_ref[1, r])
        steps.append(jnp.where(inside, softplus(raw + bias), 0.0))
    step = jnp.concatenate(steps, axis=0)
    log2_decay = step * jnp.concatenate([rate] * group, axis=0)
    both = exact_dot(log2_decay, tri)
    run, tot = both[:, :Q], both[:, Q:]
    key = jnp.minimum(run - jnp.log(step) * LOG2E, 1e30)
    left = jnp.exp2(tot - run) * step
    run_parts, key_parts, grown_parts = (
        [p.astype(F32) for p in three_parts(a)] for a in (run, key, jnp.exp2(run))
    )
    ones = jnp.ones((H, Q), F32)
    row = lax.broadcasted_iota(jnp.int32, (4 * H, Q), 0)
    for k in range(group):
        c = g * group + k
        at = slice(k * H, (k + 1) * H)
        parts = [p[at] for p in run_parts] + [ones] + [p[at] for p in grown_parts] + [jnp.zeros_like(ones)]
        cols_ref[c] = jnp.concatenate(parts, axis=0).astype(BF16)
        for h in range(H):
            block = jnp.where((row < 3 * H) & (row % H == h), 1.0, 0.0)
            for i, p in enumerate(key_parts):
                block = jnp.where(row == 3 * H + i, -p[k * H + h : k * H + h + 1], block)
            gaps_ref[c, :, h * Q : (h + 1) * Q] = block.astype(BF16)
        rows_ref[c] = left[at]
        sums_ref[c] = jnp.concatenate([tot[at], total], axis=0)
        total = total + tot[at]
    return total


def triangle():
    i = lax.broadcasted_iota(jnp.int32, (Q, 2 * Q), 0)
    j = lax.broadcasted_iota(jnp.int32, (Q, 2 * Q), 1)
    return jnp.where((i <= j), 1.0, 0.0).astype(BF16)


def per_head_lanes(rows, k):
    lane = lax.broadcasted_iota(jnp.int32, (1, 2 * W), 1)
    pieces = [
        jnp.where(lane < W, rows[k + 2 * p : k + 2 * p + 1], rows[k + 2 * p + 1 : k + 2 * p + 2])
        for p in range(H // 2)
    ]
    return jnp.concatenate(pieces, axis=1)


def split_pair(x, p):
    lane = lax.broadcasted_iota(jnp.int32, (Q, 2 * W), 1)
    pair = x[:, 2 * W * p : 2 * W * (p + 1)]
    zero = jnp.zeros_like(pair)
    return jnp.concatenate([jnp.where(lane < W, pair, zero), jnp.where(lane < W, zero, pair)], axis=0)


def fresh_state(bt, left, pairs):
    b = bt.astype(F32)
    out = []
    for p in range(H // 2):
        scaled = [(b * left[h : h + 1]).astype(BF16) for h in (2 * p, 2 * p + 1)]
        out.append(jnp.dot(jnp.concatenate(scaled, axis=1), pairs[p], preferred_element_type=F32))
    return jnp.concatenate(out, axis=1)


def row_per_head(values):
    row = lax.broadcasted_iota(jnp.int32, (H, Q), 0)
    out = jnp.full((H, Q), values[0], F32)
    for h in range(1, H):
        out = jnp.where(row == h, values[h], out)
    return out


def join(states, totals, me):
    count = len(states)
    before = before_log = whole = whole_log = 0.0
    reach = jnp.zeros_like(totals[0])
    after = jnp.zeros_like(totals[0])
    for k in reversed(range(count)):
        is_before = k < me
        weight = jnp.where(is_before, jnp.exp2(reach), 0.0)
        before = before + per_head_lanes(weight, 0) * states[k]
        whole = whole + per_head_lanes(jnp.exp2(after), 0) * states[k]
        reach = reach + jnp.where(is_before, totals[k], 0.0)
        after = after + totals[k]
    return (reach, before), (after, whole)


def main_kernel(
    x_hbm,
    gate_hbm,
    b_hbm,
    c_hbm,
    raw_hbm,
    bias_smem,
    decay_smem,
    skip_smem,
    tissue_ref,
    gated_hbm,
    scale_ref,
    raw_ref,
    x_ref,
    gate_ref,
    y_ref,
    silu_ref,
    starts,
    gated_ref,
    maps,
    cols_ref,
    gaps_ref,
    ct_ref,
    rows_ref,
    sums_ref,
    state_ref,
    squares,
    core_s,
    core_l,
    y_s,
    y_l,
    z_s,
    z_l,
    local_sem,
    load_sem,
    gate_sem,
    out_sem,
    map_send,
    map_recv,
    near_send,
    near_recv,
    far_send,
    far_recv,
    sq_send,
    sq_recv,
):
    tokens = x_ref.shape[0]
    chunks = tokens // Q
    per_seg = chunks // SEGS
    seg = tokens // SEGS
    z, yy, core, me = (lax.axis_index(a) for a in (*SEQ, "chan"))
    around = lax.axis_size("chan")

    def map_load(a, g):
        at = pl.ds(g * seg, seg)
        return pltpu.make_async_copy((b_hbm, c_hbm)[a].at[:, at], maps.at[a, 0, g], load_sem.at[a, g])

    load_x = pltpu.make_async_copy(x_hbm, x_ref, local_sem.at[0])
    load_raw = pltpu.make_async_copy(raw_hbm, raw_ref, local_sem.at[1])

    def gate_load(g):
        at = pl.ds(pl.multiple_of(g * seg, Q), seg)
        return pltpu.make_async_copy(gate_hbm.at[at, :], gate_ref.at[lax.rem(g, 2)], gate_sem.at[g])

    for g in range(SEGS):
        map_load(0, g).start()
    load_raw.start()
    squares[me] = jnp.zeros_like(squares[0])

    barrier = pltpu.get_barrier_semaphore()
    peers = [{"chan": lax.rem(me + d, around)} for d in (1, 2, 3)]
    peers += [{"seq_1": lax.rem(yy + d, 4)} for d in (1, 2, 3)]
    peers += [{"seq_0": lax.rem(z + d, 4)} for d in (1, 2, 3)]
    peers += [{"seq_2": 1 - core}]
    for peer in peers:
        pl.semaphore_signal(barrier, inc=1, device_id=peer, device_id_type=MESH)
    pl.semaphore_wait(barrier, len(peers))

    def remote(src, dst, send, recv, peer):
        return pltpu.make_async_remote_copy(
            src_ref=src, dst_ref=dst, send_sem=send, recv_sem=recv, device_id=peer, device_id_type=MESH
        )

    def own_copy(side, j):
        a, g = j // SEGS, lax.rem(j, SEGS)
        peer = {"chan": lax.rem(me + 1 + 2 * side, around)}
        return remote(
            maps.at[a, 0, g], maps.at[a, 1 + side, g], map_send.at[side, j], map_recv.at[side, j], peer
        )

    def far_copy(side, j):
        a, g = j // SEGS, lax.rem(j, SEGS)
        half = maps.shape[3] // 2
        at = slice(side * half, (side + 1) * half)
        peer = {"chan": lax.rem(me + 1 + 2 * side, around)}
        return remote(
            maps.at[a, 1 + side, g, at], maps.at[a, 3, g, at], map_send.at[2 + side, j], map_recv.at[2 + side, j], peer
        )

    def send_own(j):
        own_copy(0, j).start()
        own_copy(1, j).start()

    def service(j):
        for side in range(2):
            own_copy(side, j).wait_recv()
            far_copy(side, j).start()

        @pl.when(j + LEAD < 2 * SEGS)
        def _():
            send_own(j + LEAD)

    def wait_far(j):
        far_copy(0, j).wait_recv()
        far_copy(1, j).wait_recv()

    for j in range(LEAD):
        map_load(0, j).wait()
        send_own(j)
    for j in range(LEAD, SEGS):
        map_load(0, j).wait()
    for g in range(SEGS):
        map_load(1, g).start()
    load_x.start()
    gate_load(0).start()
    gate_load(1).start()
    load_raw.wait()
    bias = row_per_head([bias_smem[h] for h in range(H)])
    rate = jnp.exp(row_per_head([decay_smem[h] for h in range(H)])) * -LOG2E
    skip = per_head_lanes(row_per_head([skip_smem[h] for h in range(H)]), 0)

    tri = triangle()
    group = 8
    total = lax.fori_loop(
        0,
        chunks // group,
        lambda g, t: decay_group(
            g, group, raw_ref, bias, rate, tissue_ref, tri, cols_ref, gaps_ref, rows_ref, sums_ref, t
        ),
        jnp.zeros((H, Q), F32),
    )
    for g in range(SEGS):
        map_load(1, g).wait()
    load_x.wait()
    state_ref[...] = jnp.zeros_like(state_ref)

    def tokens_of(c):
        return pl.ds(pl.multiple_of(c * Q, Q), Q)

    def map_of(a, c):
        g = c // per_seg
        return maps[a, :, g, :, tokens_of(c - g * per_seg)].reshape(N, Q)

    def band_some(g, i):
        fresh, decay, silu, direct = [], [], [], []
        for k in range(BAND):
            c = g * per_seg + i * BAND + k
            rows = rows_ref[c]
            x = x_ref[tokens_of(c), :]
            pairs = [split_pair(x, p) for p in range(H // 2)]
            fresh.append(fresh_state(map_of(0, c), rows, pairs))
            decay.append(jnp.exp2(per_head_lanes(sums_ref[c], 0)))
            gate = gate_ref[lax.rem(g, 2), tokens_of(i * BAND + k), :].astype(F32) * 0.5
            silu.append(gate + gate * jnp.tanh(gate))
            direct.append(skip * x.astype(F32))
        state = state_ref[...]
        states = []
        for k in range(BAND):
            states.append(state)
            state = decay[k] * state + fresh[k]
        state_ref[...] = state
        for k in range(BAND):
            c = g * per_seg + i * BAND + k
            starts[c] = states[k]
            silu_ref[tokens_of(c), :] = silu[k]
            y_ref[tokens_of(c), :] = direct[k]

    def band_seg(g):
        gate_load(g).wait()
        lax.fori_loop(0, per_seg // BAND, lambda i, carry: (band_some(g, i), carry)[1], 0)

        @pl.when(g + 2 < SEGS)
        def _():
            gate_load(g + 2).start()

    def intra_some(g, i):
        t = lax.broadcasted_iota(jnp.int32, (Q, Q), 0)
        s = lax.broadcasted_iota(jnp.int32, (Q, Q), 1)
        def ahead(k):
            c = g * per_seg + i * INTRA + k
            cm = map_of(1, c).T
            gap = jnp.dot(cols_ref[c, : 4 * H, :].T, gaps_ref[c], preferred_element_type=F32)
            scores = jnp.dot(cm, map_of(0, c), preferred_element_type=F32)
            return cm, scores, gap

        coming = [ahead(0), ahead(1)]
        for k in range(INTRA):
            c = g * per_seg + i * INTRA + k
            if k + 2 < INTRA:
                coming.append(ahead(k + 2))
            cm, scores, gap = coming[k]
            ct_ref[tokens_of(c), :] = cm
            x = x_ref[tokens_of(c), :]
            scores = jnp.where(t >= s, scores, 0.0)
            inner = []
            for p in range(H // 2):
                damp = jnp.exp2(jnp.minimum(gap[:, 2 * p * Q : 2 * (p + 1) * Q], 127.0))
                weights = [(scores * damp[:, h * Q : (h + 1) * Q]).astype(BF16) for h in range(2)]
                inner.append(
                    jnp.dot(jnp.concatenate(weights, axis=1), split_pair(x, p), preferred_element_type=F32)
                )
            y_ref[tokens_of(c), :] += jnp.concatenate(inner, axis=1)

    def intra_seg(g):
        lax.fori_loop(0, per_seg // INTRA, lambda i, carry: (intra_some(g, i), carry)[1], 0)

    def finish_some(g, i):
        out, sums_out = [], []
        entering = state_ref[...]
        row = lax.broadcasted_iota(jnp.int32, (4 * H, H * W), 0)
        lane = lax.broadcasted_iota(jnp.int32, (4 * H, H * W), 1)
        spread = jnp.where((row < 3 * H) & (row % H == lane // W), 1.0, 0.0).astype(BF16)
        for k in range(FINISH):
            c = g * per_seg + i * FINISH + k
            at = tokens_of(c)
            state = starts[c] + jnp.exp2(per_head_lanes(sums_ref[c], H)) * entering
            carried = jnp.dot(ct_ref[at, :], state.astype(BF16), preferred_element_type=F32)
            grown = jnp.dot(cols_ref[c, 4 * H :, :].T, spread, preferred_element_type=F32)
            gated = (y_ref[at, :] + grown * carried) * silu_ref[at, :]
            out.append(gated.astype(BF16))
            square = gated * gated
            square = square[:, :Q] + square[:, Q:]
            sums_out.append(jnp.sum(square.T, axis=0, keepdims=True))
        for k in range(FINISH):
            gated_ref[lax.rem(g, 2), tokens_of(i * FINISH + k), :] = out[k]
            squares[me, g, pl.ds(i * FINISH + k, 1), :] = sums_out[k]

    def gated_copy(g):
        at = pl.ds(pl.multiple_of(g * seg, Q), seg)
        return pltpu.make_async_copy(gated_ref.at[lax.rem(g, 2)], gated_hbm.at[at, :], out_sem.at[g])

    def square_copies(g):
        return [
            remote(
                squares.at[me, g],
                squares.at[me, g],
                sq_send.at[d - 1, g],
                sq_recv.at[d - 1, g],
                {"chan": lax.rem(me + d, around)},
            )
            for d in (1, 2, 3)
        ]

    def finish_seg(g):
        @pl.when(g >= 2)
        def _():
            gated_copy(g - 2).wait()

        lax.fori_loop(0, per_seg // FINISH, lambda i, carry: (finish_some(g, i), carry)[1], 0)
        gated_copy(g).start()
        for copy in square_copies(g):
            copy.start()

    def exchange(slots_s, slots_l, sends, recvs, axis, at):
        size = slots_s.shape[0]
        copies = []
        for d in range(1, size):
            peer = {axis: lax.rem(at + d, size)}
            copies.append(remote(slots_s.at[at], slots_s.at[at], sends(d, 0), recvs(d, 0), peer))
            copies.append(remote(slots_l.at[at], slots_l.at[at], sends(d, 1), recvs(d, 1), peer))
        return copies

    def put(slots_s, slots_l, at, pair):
        slots_l[at] = pair[0]
        slots_s[at] = pair[1].astype(slots_s.dtype)

    def get(slots_s, slots_l, at):
        size = slots_s.shape[0]
        return join([slots_s[k].astype(F32) for k in range(size)], [slots_l[k] for k in range(size)], at)

    service(0)

    def band_step(j, carry):
        service(j)
        wait_far(j - 1)
        band_seg(j - 1)
        return carry

    lax.fori_loop(1, SEGS + 1, band_step, 0)

    near = exchange(core_s, core_l, lambda d, k: near_send.at[k], lambda d, k: near_recv.at[k], "seq_2", core)
    along_y = exchange(
        y_s, y_l, lambda d, k: far_send.at[0, d - 1, k], lambda d, k: far_recv.at[0, d - 1, k], "seq_1", yy
    )
    along_z = exchange(
        z_s, z_l, lambda d, k: far_send.at[1, d - 1, k], lambda d, k: far_recv.at[1, d - 1, k], "seq_0", z
    )

    def inner_step(g, carry=0):
        service(SEGS + g + 1)
        wait_far(SEGS + g)
        intra_seg(g)
        return carry

    def finish_step(g, carry=0):
        finish_seg(g)
        return carry

    put(core_s, core_l, core, (total, state_ref[...]))
    for copy in near:
        copy.start()
    inner_step(0)
    for copy in near:
        copy.wait()
    in_core, chip = get(core_s, core_l, core)
    put(y_s, y_l, yy, chip)
    for copy in along_y:
        copy.start()
    lax.fori_loop(1, 3, inner_step, 0)
    for copy in along_y:
        copy.wait()
    in_y, plane = get(y_s, y_l, yy)
    put(z_s, z_l, z, plane)
    for copy in along_z:
        copy.start()
    lax.fori_loop(3, 5, inner_step, 0)
    for copy in along_z:
        copy.wait()
    in_z, _ = get(z_s, z_l, z)
    lanes = lambda log: per_head_lanes(jnp.exp2(log), 0)
    state_ref[...] = lanes(in_core[0]) * (lanes(in_y[0]) * in_z[1] + in_y[1]) + in_core[1]

    finish_seg(0)
    inner_step(5)
    lax.fori_loop(1, 3, finish_step, 0)
    inner_step(6)
    lax.fori_loop(3, 7, finish_step, 0)
    wait_far(2 * SEGS - 1)
    intra_seg(SEGS - 1)
    finish_seg(SEGS - 1)

    def close(g, carry):
        for copy in square_copies(g):
            copy.wait()
        mean = (squares[0, g] + squares[1, g] + squares[2, g] + squares[3, g]) / D
        scale_ref[g] = lax.rsqrt(mean + EPS)
        return carry

    lax.fori_loop(0, SEGS, close, 0)
    gated_copy(SEGS - 2).wait()
    gated_copy(SEGS - 1).wait()

    def drain(j, carry):
        own_copy(0, j).wait_send()
        own_copy(1, j).wait_send()
        far_copy(0, j).wait_send()
        far_copy(1, j).wait_send()
        return carry

    lax.fori_loop(0, 2 * SEGS, drain, 0)


def norm_kernel(gated_hbm, scale_ref, gain_ref, out_hbm, gated_ref, out_ref, load_sem, store_sem):
    seg = gated_ref.shape[0] // SEGS

    def load(g):
        at = pl.ds(g * seg, seg)
        return pltpu.make_async_copy(gated_hbm.at[at, :], gated_ref.at[at, :], load_sem.at[g])

    def store(g):
        at = pl.ds(g * seg, seg)
        return pltpu.make_async_copy(out_ref.at[at, :], out_hbm.at[at, :], store_sem.at[g])

    for g in range(SEGS):
        load(g).start()

    def one(g, carry):
        col = scale_ref[g].T
        load(g).wait()
        for k in range(seg // Q):
            at = pl.ds(pl.multiple_of(g * seg + k * Q, Q), Q)
            out_ref[at, :] = (gated_ref[at, :].astype(F32) * col[:, k : k + 1] * gain_ref[...]).astype(BF16)
        store(g).start()
        return carry

    lax.fori_loop(0, SEGS, one, 0)
    for g in range(SEGS):
        store(g).wait()


def per_device(
    features, gate_input, input_map, output_map, step_raw, step_bias, decay_log, skip_gain, norm_gain, tissue
):
    tokens, width = features.shape
    chunks = tokens // Q
    vmem = pl.BlockSpec(memory_space=pltpu.VMEM)
    hbm = pl.BlockSpec(memory_space=pl.ANY)
    around = lax.axis_size("chan")
    dma = pltpu.SemaphoreType.DMA
    slots = lambda n, dtype: [pltpu.VMEM((n, N, width), dtype), pltpu.VMEM((n, H, Q), F32)]
    gated, scale = pl.pallas_call(
        main_kernel,
        out_shape=(
            jax.ShapeDtypeStruct((tokens, width), BF16),
            jax.ShapeDtypeStruct((SEGS, 16, Q), F32),
        ),
        in_specs=[hbm] * 5 + [pl.BlockSpec(memory_space=pltpu.SMEM)] * 4,
        out_specs=(hbm, vmem),
        scratch_shapes=[
            pltpu.VMEM((H, tokens), F32),
            pltpu.VMEM((tokens, width), BF16),
            pltpu.VMEM((2, tokens // SEGS, width), BF16),
            pltpu.VMEM((tokens, width), F32),
            pltpu.VMEM((tokens, width), F32),
            pltpu.VMEM((chunks, N, width), F32),
            pltpu.VMEM((2, tokens // SEGS, width), BF16),
            pltpu.VMEM((2, around, SEGS, N // around, tokens // SEGS), BF16),
            pltpu.VMEM((chunks, 8 * H, Q), BF16),
            pltpu.VMEM((chunks, 4 * H, H * Q), BF16),
            pltpu.VMEM((tokens, N), BF16),
            pltpu.VMEM((chunks, H, Q), F32),
            pltpu.VMEM((chunks, 2 * H, Q), F32),
            pltpu.VMEM((N, width), F32),
            pltpu.VMEM((around, SEGS, 16, Q), F32),
            *slots(2, F32),
            *slots(4, BF16),
            *slots(4, BF16),
            dma((2,)),
            dma((2, SEGS)),
            dma((SEGS,)),
            dma((SEGS,)),
            dma((4, 2 * SEGS)),
            dma((4, 2 * SEGS)),
            dma((2,)),
            dma((2,)),
            dma((2, 3, 2)),
            dma((2, 3, 2)),
            dma((3, SEGS)),
            dma((3, SEGS)),
        ],
        compiler_params=pltpu.CompilerParams(
            collective_id=0, has_side_effects=True, vmem_limit_bytes=67043328
        ),
        name="scan",
    )(features, gate_input, input_map.T, output_map.T, step_raw.T, step_bias, decay_log, skip_gain, tissue.T)
    return pl.pallas_call(
        norm_kernel,
        out_shape=jax.ShapeDtypeStruct((tokens, width), BF16),
        in_specs=[hbm, vmem, vmem],
        out_specs=hbm,
        scratch_shapes=[
            pltpu.VMEM((tokens, width), BF16),
            pltpu.VMEM((tokens, width), BF16),
            dma((SEGS,)),
            dma((SEGS,)),
        ],
        compiler_params=pltpu.CompilerParams(vmem_limit_bytes=63 * 1024 * 1024),
        name="norm",
    )(gated, scale, norm_gain[None, :])


def solution(mesh):
    split = Mesh(mesh.devices.reshape(4, 4, 2, mesh.shape["chan"]), (*SEQ, "chan"))
    tokens = P(SEQ, "chan")
    placed = (tokens,) * 5 + (P("chan"),) * 4 + (P(SEQ, None),)
    return jax.shard_map(per_device, mesh=split, in_specs=placed, out_specs=tokens, check_vma=False)
```
